32 devices in a mesh: seq: 16 (over z, y, x), tp: 2 (over core).
Axes of the slice: x: 2, y: 2, z: 4, core: 2. Of those that a mesh axis runs over, the one named last changes fastest.
Arguments:
- tokens: bfloat16 [8192, 2048], P('seq', 'tp'), may hold values from -6 to 6
- ln_gain: bfloat16 [2048], replicated, may hold values from 0.5 to 4.1
- w_qkv: bfloat16 [3, 2048, 2048], P(None, None, 'tp'), may hold values from -0.15467961 to 0.15467961
- w_out: bfloat16 [2048, 2048], P('tp'), may hold values from -0.1875 to 0.1875
Outputs:
- mixed: bfloat16 [8192, 2048], P('seq', 'tp')
The draws below stay inside these ranges and needn't reach their ends.
All inputs are finite; a program needn't handle non-finite values.
Results may differ from the reference program's by a relative error of at most 0.011.
Values may be sent and summed in bfloat16 or wider, within the bound.
A program may use at most 256 MiB of HBM per device.

```python
import jax
import jax.numpy as jnp
from jax import lax

D = 2048
HEADS = 16
HEAD_DIM = 128
SEQ = 8192


def draw_ln_gain(key, part):
    return jax.random.uniform(key, (D,), jnp.float32, 0.6, 1.4).astype(jnp.bfloat16)


def draw_tokens(key, part):
    normal_rows = jnp.clip(jax.random.normal(jax.random.fold_in(key, 11), (SEQ, D), jnp.float32), -6.0, 6.0)
    return normal_rows.astype(jnp.bfloat16)


def draw_w_qkv(key, part):
    bound_abs = 7.0 * D ** (-0.5)
    entries = jnp.clip(jax.random.normal(jax.random.fold_in(key, 23), (3, D, HEADS * HEAD_DIM), jnp.float32), -6.0, 6.0) * D ** (-0.5)
    return jnp.clip(entries, -bound_abs, bound_abs).astype(jnp.bfloat16)


def spiked(values, rng, source, target, parts, factor):
    def block_of(dim):
        return (jnp.arange(values.shape[dim]) // (values.shape[dim] // parts)).reshape((-1,) + (1,) * (values.ndim - 1 - dim))

    one_side = jax.random.permutation(rng, parts)[block_of(target)]
    other_side = (block_of(target) + parts // 2) % parts
    return jnp.where((block_of(source) == one_side) | (block_of(source) == other_side), factor * values, values)


def shard_levels(rng, shape, cuts, least, top_value):
    gain, own = 1.0, jax.random.fold_in(rng, 6)
    for axis_at, parts in cuts:
        draws = jnp.exp(jax.random.uniform(jax.random.fold_in(own, axis_at), (parts,), jnp.float32, least / len(cuts), top_value / len(cuts)))
        gain = gain * jnp.repeat(draws, shape[axis_at] // parts).reshape([-1 if axis == axis_at else 1 for axis in range(len(shape))])
    return gain


def gaussian_with(stream_key, shape, scale, most, split, heavy, kind=jnp.bfloat16):
    result = scale * jax.random.normal(stream_key, shape, jnp.float32)
    if split:
        result = result * shard_levels(stream_key, shape, split, -0.22, 0.18)
    return jnp.clip(spiked(result, jax.random.fold_in(stream_key, 3), *heavy), -most, most).astype(kind)


def setup_inputs(seed: int = 0) -> dict:
    seeds = jax.random.split(jax.random.key(seed), 5)
    return {
        "tokens": draw_tokens(jax.random.fold_in(seeds[4], 71), 0),
        "ln_gain": draw_ln_gain(jax.random.fold_in(seeds[4], 71), 0),
        "w_qkv": draw_w_qkv(jax.random.fold_in(seeds[4], 71), 0),
        "w_out": gaussian_with(seeds[3], (HEADS * HEAD_DIM, D), (HEADS * HEAD_DIM) ** -0.5, 0.1875, ((0, 2),), (0, 1, 2, 2.0)),
    }


def reference(tokens, ln_gain, w_qkv, w_out):
    values = tokens.astype(jnp.float32)
    average = lax.optimization_barrier(jnp.mean(values, axis=1, keepdims=True))
    second = lax.optimization_barrier(jnp.mean(values * values, axis=1, keepdims=True))
    normed = ((values - average) * lax.rsqrt(second - average * average + 1e-06) * ln_gain.astype(jnp.float32)).astype(jnp.bfloat16)
    queries = jnp.dot(normed, w_qkv[0], preferred_element_type=jnp.float32).astype(jnp.bfloat16).reshape(SEQ, HEADS, HEAD_DIM)
    keys_all = jnp.dot(normed, w_qkv[1], preferred_element_type=jnp.float32).astype(jnp.bfloat16).reshape(SEQ, HEADS, HEAD_DIM)
    vals_all = jnp.dot(normed, w_qkv[2], preferred_element_type=jnp.float32).astype(jnp.bfloat16).reshape(SEQ, HEADS, HEAD_DIM)
    span = min(512, SEQ)
    factor = HEAD_DIM ** (-0.5)
    keys_wide = keys_all.astype(jnp.float32)
    vals_wide = vals_all.astype(jnp.float32)

    def attend(offset):
        query_block = lax.dynamic_slice_in_dim(queries, offset, span, 0).astype(jnp.float32)
        scores = jnp.einsum('thc,shc->ths', query_block, keys_wide) * factor
        highest = lax.optimization_barrier(jnp.max(scores, axis=2, keepdims=True))
        expon = jnp.exp(scores - highest)
        denoms = lax.optimization_barrier(jnp.sum(expon, axis=2))
        weights = expon.astype(jnp.bfloat16).astype(jnp.float32)
        summed = jnp.einsum('ths,shc->thc', weights, vals_wide) / denoms[:, :, None]
        return summed.reshape(span, HEADS * HEAD_DIM).astype(jnp.bfloat16)
    offsets = jnp.arange(SEQ // span, dtype=jnp.int32) * span
    context = lax.map(attend, offsets).reshape(SEQ, HEADS * HEAD_DIM)
    projected = jnp.dot(context, w_out, preferred_element_type=jnp.float32)
    return (values + projected).astype(jnp.bfloat16)
```

```python
import functools
import math

import jax
import jax.numpy as jnp
from jax import lax
from jax.experimental import pallas as pl
from jax.experimental.pallas import tpu as pltpu
from jax.sharding import PartitionSpec as P

HEAD_DIM = 128
MESH = pl.DeviceIdType.MESH
ANY = pl.BlockSpec(memory_space=pl.ANY)


def remote(src, dst, send, recv, seq, tp):
    return pltpu.make_async_remote_copy(
        src_ref=src, dst_ref=dst, send_sem=send, recv_sem=recv, device_id=(seq, tp), device_id_type=MESH
    )


def put(src, dst, send, recv, seq, tp, own):
    @pl.when(own)
    def _():
        pltpu.make_async_copy(src, dst, recv).start()

    @pl.when(jnp.logical_not(own))
    def _():
        remote(src, dst, send, recv, seq, tp).start()


def project_kernel(
    n, heads, tok, gain, w, q_out, kv_out,
    pair, normed, wbuf, xq, xkv, wsem, psem, qsend, kvsend, qrecv, kvrecv, fsend, frecv,
):
    me, core = lax.axis_index("seq"), lax.axis_index("tp")
    other = 1 - core
    rows, feats = tok.shape
    half = rows // 2
    blocks = heads // 2
    width = 2 * HEAD_DIM

    mine = pltpu.make_async_copy(tok, pair.at[core], psem.at[0])
    mine.start()
    swap = remote(tok, pair.at[core], psem.at[1], psem.at[2], me, other)
    swap.start()

    def wcopy(b, j):
        return pltpu.make_async_copy(w.at[j, :, pl.ds(pl.multiple_of(b * width, width), width)], wbuf.at[b, j], wsem.at[b, j])

    def fetch(b, carry):
        for j in range(3):
            wcopy(b, j).start()
        return carry

    lax.fori_loop(0, blocks, fetch, 0)
    mine.wait()
    swap.wait()

    step = 32

    def norm(i, carry):
        at = pl.ds(pl.multiple_of(i * step, step), step)
        a = pair[0, at, :].astype(jnp.float32)
        b = pair[1, at, :].astype(jnp.float32)
        average = (jnp.sum(a, axis=1, keepdims=True) + jnp.sum(b, axis=1, keepdims=True)) / (2 * feats)
        second = (jnp.sum(a * a, axis=1, keepdims=True) + jnp.sum(b * b, axis=1, keepdims=True)) / (2 * feats)
        scale = lax.rsqrt(second - average * average + 1e-06)
        normed[at, :feats] = ((a - average) * scale * gain[0:1, :feats]).astype(jnp.bfloat16)
        normed[at, feats:] = ((b - average) * scale * gain[0:1, feats:]).astype(jnp.bfloat16)
        return carry

    lax.fori_loop(0, rows // step, norm, 0)

    def sends(h, wait):
        chip = core * heads + h
        for u in range(2):
            own = jnp.logical_and(chip == me, core == u)
            at = pl.ds(u * half, half)
            args_q = (xq.at[h, at], q_out.at[me], qsend.at[h, u], qrecv.at[me], chip, u)
            args_kv = (xkv.at[h, at], kv_out.at[u, me], kvsend.at[h, u], kvrecv.at[me], chip, u)
            if wait:

                @pl.when(jnp.logical_not(own))
                def _():
                    remote(*args_q).wait_send()
                    remote(*args_kv).wait_send()
            else:
                put(*args_kv, own)
                put(*args_q, own)

    factor = HEAD_DIM ** (-0.5) * math.log2(math.e)

    def project(b, carry):
        for j in range(3):
            wcopy(b, j).wait()
            got = jnp.dot(normed[...], wbuf[b, j], preferred_element_type=jnp.float32)
            if j == 0:
                got = got * factor
            got = got.astype(jnp.bfloat16)
            for i in range(2):
                part = got[:, i * HEAD_DIM : (i + 1) * HEAD_DIM]
                if j == 0:
                    xq[2 * b + i] = part
                else:
                    xkv[2 * b + i, :, (j - 1) * HEAD_DIM : j * HEAD_DIM] = part

        @pl.when(b > 0)
        def _():
            sends(2 * b - 2, False)
            sends(2 * b - 1, False)

        return carry

    lax.fori_loop(0, blocks, project, 0)
    sends(2 * blocks - 2, False)
    sends(2 * blocks - 1, False)

    def got_kv(s):
        return remote(xkv.at[0, pl.ds(0, half)], kv_out.at[core, s], kvsend.at[0, 0], kvrecv.at[s], me, other)

    def forward(s):
        return remote(kv_out.at[core, s], kv_out.at[core, s], fsend.at[s], frecv.at[s], me, other)

    def pass_on(i, carry):
        s = lax.rem(me + i, n)
        got_kv(s).wait_recv()
        forward(s).start()
        return carry

    lax.fori_loop(0, n, pass_on, 0)

    def finish(s, carry):
        remote(xq.at[0, pl.ds(0, half)], q_out.at[s], qsend.at[0, 0], qrecv.at[s], me, other).wait_recv()
        forward(s).wait_send()
        remote(kv_out.at[other, s], kv_out.at[other, s], fsend.at[s], frecv.at[s], me, other).wait_recv()
        return carry

    lax.fori_loop(0, n, finish, 0)

    def drain(h, carry):
        sends(h, True)
        return carry

    lax.fori_loop(0, heads, drain, 0)


def project(tokens, gain, w_qkv, n):
    rows, feats = tokens.shape
    heads = w_qkv.shape[2] // HEAD_DIM
    half = rows // 2
    bf = jnp.bfloat16
    dma = pltpu.SemaphoreType.DMA
    return pl.pallas_call(
        functools.partial(project_kernel, n, heads),
        out_shape=(
            jax.ShapeDtypeStruct((n, half, HEAD_DIM), bf),
            jax.ShapeDtypeStruct((2, n, half, 2 * HEAD_DIM), bf),
        ),
        in_specs=[ANY, pl.BlockSpec(memory_space=pltpu.VMEM), ANY],
        out_specs=(ANY, ANY),
        scratch_shapes=[
            pltpu.VMEM((2, rows, feats), bf),
            pltpu.VMEM((rows, 2 * feats), bf),
            pltpu.VMEM((heads // 2, 3, 2 * feats, 2 * HEAD_DIM), bf),
            pltpu.VMEM((heads, rows, HEAD_DIM), bf),
            pltpu.VMEM((heads, rows, 2 * HEAD_DIM), bf),
            dma((heads // 2, 3)), dma((3,)), dma((heads, 2)), dma((heads, 2)),
            dma((n,)), dma((n,)), dma((n,)), dma((n,)),
        ],
        compiler_params=pltpu.CompilerParams(has_side_effects=True, vmem_limit_bytes=48 * 1024 * 1024),
        name="project",
    )(tokens, gain, w_qkv)


def attend_kernel(chunk, group, q_ref, kv_ref, out_ref, vones):
    keys = kv_ref.shape[0]

    @pl.when(pl.program_id(0) == 0)
    def _():
        vones[:, :HEAD_DIM] = kv_ref[:, HEAD_DIM:]
        vones[:, HEAD_DIM:] = jnp.ones((keys, HEAD_DIM), jnp.bfloat16)

    parts = q_ref.shape[0] // group
    queries = [q_ref[g * group : (g + 1) * group, :] for g in range(parts)]

    def body(i, carry):
        at = pl.ds(pl.multiple_of(i * chunk, chunk), chunk)
        kept = []
        scores = [
            lax.dot_general(q, kv_ref[at, :HEAD_DIM], (((1,), (1,)), ((), ())), preferred_element_type=jnp.float32)
            for q in queries
        ]
        for (top, total), s in zip(carry, scores):
            high = jnp.maximum(top, jnp.max(s, axis=1, keepdims=True))
            p = jnp.exp2((s - high).astype(jnp.bfloat16))
            add = jnp.dot(p, vones[at, :], preferred_element_type=jnp.float32)
            kept.append((high, total * jnp.exp2(top - high) + add))
        return tuple(kept)

    start = tuple(
        (jnp.full((group, 1), -1e30, jnp.float32), jnp.zeros((group, 2 * HEAD_DIM), jnp.float32)) for _ in queries
    )
    done = lax.fori_loop(0, keys // chunk, body, start, unroll=2)
    for g, (_, total) in enumerate(done):
        out_ref[g * group : (g + 1) * group, :] = (total[:, :HEAD_DIM] / total[:, HEAD_DIM:]).astype(jnp.bfloat16)


def attend(q, kv, block=512, group=256, chunk=1024):
    count, keys = q.shape[0], kv.shape[0]
    block = math.gcd(block, count)
    group = math.gcd(group, block)
    chunk = math.gcd(chunk, keys)
    return pl.pallas_call(
        functools.partial(attend_kernel, chunk, group),
        grid=(count // block,),
        out_shape=jax.ShapeDtypeStruct((count, HEAD_DIM), jnp.bfloat16),
        in_specs=[
            pl.BlockSpec((block, HEAD_DIM), lambda i: (i, 0)),
            pl.BlockSpec((keys, 2 * HEAD_DIM), lambda i: (0, 0)),
        ],
        out_specs=pl.BlockSpec((block, HEAD_DIM), lambda i: (i, 0)),
        scratch_shapes=[pltpu.VMEM((keys, 2 * HEAD_DIM), jnp.bfloat16)],
        compiler_params=pltpu.CompilerParams(
            dimension_semantics=("arbitrary",), vmem_limit_bytes=48 * 1024 * 1024
        ),
        name="attend",
    )(q, kv)


def output_kernel(n, heads, ctx, tok, w, out, held, sent, came, send, recv, psem):
    me, core = lax.axis_index("seq"), lax.axis_index("tp")
    other = 1 - core
    rows, feats = tok.shape
    half = rows // 2
    home, slot = me // heads, lax.rem(me, heads)

    def place(u, h):
        return held.at[
            pl.ds(pl.multiple_of(u * half, half), half), pl.ds(pl.multiple_of(h * HEAD_DIM, HEAD_DIM), HEAD_DIM)
        ]

    def give(i, wait):
        s = lax.rem(me + i, n)
        own = jnp.logical_and(s == me, home == core)
        args = (ctx.at[s], place(core, slot), send.at[s], recv.at[core, slot], s, home)
        if wait:

            @pl.when(jnp.logical_not(own))
            def _():
                remote(*args).wait_send()
        else:
            put(*args, own)

    def start(i, carry):
        give(i, False)
        return carry

    lax.fori_loop(0, n, start, 0)

    def arrive(i, carry):
        u, h = i // heads, lax.rem(i, heads)
        remote(ctx.at[0], place(u, h), send.at[0], recv.at[u, h], me, other).wait_recv()
        return carry

    lax.fori_loop(0, 2 * heads, arrive, 0)

    width = 2 * HEAD_DIM

    def product(side, i):
        at = pl.ds(pl.multiple_of(side * feats + i * width, width), width)
        return jnp.dot(held[...], w[:, at], preferred_element_type=jnp.float32)

    pieces = feats // width

    def share(i):
        return remote(sent.at[i], came.at[i], psem.at[0, i], psem.at[1, i], me, other)

    def theirs(i, carry):
        sent[i] = product(other, i).astype(jnp.bfloat16)

        @pl.when(i > 0)
        def _():
            share(i - 1).start()

        return carry

    lax.fori_loop(0, pieces, theirs, 0)
    share(pieces - 1).start()

    def ours(i, carry):
        at = pl.ds(pl.multiple_of(i * width, width), width)
        got = product(core, i)
        share(i).wait_recv()
        out[:, at] = (tok[:, at].astype(jnp.float32) + (got + came[i].astype(jnp.float32))).astype(jnp.bfloat16)
        return carry

    lax.fori_loop(0, pieces, ours, 0)

    def drain(i, carry):
        give(i, True)
        return carry

    lax.fori_loop(0, n, drain, 0)
    for i in range(pieces):
        share(i).wait_send()


def output(ctx, tokens, w_out, n):
    rows, feats = tokens.shape
    heads = w_out.shape[0] // HEAD_DIM
    bf = jnp.bfloat16
    dma = pltpu.SemaphoreType.DMA
    vm = pl.BlockSpec(memory_space=pltpu.VMEM)
    pieces = feats // (2 * HEAD_DIM)
    return pl.pallas_call(
        functools.partial(output_kernel, n, heads),
        out_shape=jax.ShapeDtypeStruct((rows, feats), bf),
        in_specs=[ANY, vm, vm],
        out_specs=vm,
        scratch_shapes=[
            pltpu.VMEM((rows, heads * HEAD_DIM), bf),
            pltpu.VMEM((pieces, rows, 2 * HEAD_DIM), bf),
            pltpu.VMEM((pieces, rows, 2 * HEAD_DIM), bf),
            dma((n,)), dma((2, heads)), dma((2, pieces)),
        ],
        compiler_params=pltpu.CompilerParams(has_side_effects=True, vmem_limit_bytes=32 * 1024 * 1024),
        name="output",
    )(ctx, tokens, w_out)


def head_per_chip(n, tokens, ln_gain, w_qkv, w_out):
    gain = ln_gain.astype(jnp.float32).reshape(1, -1)
    q, kv = project(tokens, gain, w_qkv, n)
    half = q.shape[1]
    ctx = attend(q.reshape(n * half, HEAD_DIM), kv.reshape(2 * n * half, 2 * HEAD_DIM))
    return output(ctx.reshape(n, half, HEAD_DIM), tokens, w_out, n)


def attend_block(totals, queries, block_kv, factor):
    running, denoms, accum = totals
    heads_here = queries.shape[1]
    keys_part = block_kv[0].reshape(block_kv.shape[1], heads_here, queries.shape[2])
    vals_part = block_kv[1].reshape(block_kv.shape[1], heads_here, queries.shape[2])
    scores = (
        jnp.einsum("thc,shc->ths", queries, keys_part, preferred_element_type=jnp.float32) * factor
    )
    highest = jnp.maximum(running, jnp.max(scores, axis=2))
    expon = jnp.exp(scores - highest[:, :, None])
    denoms = jnp.sum(expon, axis=2)
    weights = expon.astype(jnp.bfloat16)
    accum = jnp.einsum("ths,shc->thc", weights, vals_part, preferred_element_type=jnp.float32)
    return (highest, denoms, accum)


def start_totals(rows, heads_count):
    return (
        jnp.full((rows, heads_count), -1e30, jnp.float32),
        jnp.zeros((rows, heads_count), jnp.float32),
        jnp.zeros((rows, heads_count, HEAD_DIM), jnp.float32),
    )


def on_device(tokens, ln_gain, w_qkv, w_out):
    tok_rows = tokens.shape[0]
    whole = lax.all_gather(tokens, "tp", axis=1, tiled=True)
    values = whole.astype(jnp.float32)
    average = jnp.mean(values, axis=1, keepdims=True)
    second = jnp.mean(values * values, axis=1, keepdims=True)
    normed = (
        (values - average)
        * lax.rsqrt(second - average * average + 1e-06)
        * ln_gain.astype(jnp.float32)
    ).astype(jnp.bfloat16)
    projected = jnp.einsum("td,jdc->jtc", normed, w_qkv, preferred_element_type=jnp.float32).astype(
        jnp.bfloat16
    )
    heads_here = w_qkv.shape[2] // HEAD_DIM
    factor = HEAD_DIM ** (-0.5)
    queries = projected[0].reshape(tok_rows, heads_here, HEAD_DIM)
    keys_vals = projected[1:3]
    initial = start_totals(tok_rows, heads_here)
    final = attend_block(
        initial, queries, lax.all_gather(keys_vals, "seq", axis=1, tiled=True), factor
    )
    context = (
        (final[2] / final[1][:, :, None])
        .reshape(tok_rows, heads_here * HEAD_DIM)
        .astype(jnp.bfloat16)
    )
    summed = lax.psum_scatter(
        lax.dot_general(
            w_out, context, (((0,), (1,)), ((), ())), preferred_element_type=jnp.float32
        ).astype(jnp.bfloat16),
        "tp",
        scatter_dimension=0,
        tiled=True,
    ).astype(jnp.float32)
    return (tokens.astype(jnp.float32) + summed.T).astype(jnp.bfloat16)


def solution(mesh):
    in_specs = (P("seq", "tp"), P(), P(None, None, "tp"), P("tp", None))
    out_specs = P("seq", "tp")
    n, cores = mesh.shape["seq"], mesh.shape["tp"]

    def run(tokens, ln_gain, w_qkv, w_out):
        heads = w_qkv.shape[2] // HEAD_DIM
        if cores == 2 and heads * cores == n and heads % 2 == 0:
            return head_per_chip(n, tokens, ln_gain, w_qkv, w_out)
        return on_device(tokens, ln_gain, w_qkv, w_out)

    return jax.shard_map(run, mesh=mesh, in_specs=in_specs, out_specs=out_specs, check_vma=False)
```
